32 devices in a mesh: rows: 8 (over z, y), cols: 4 (over x, core).
Axes of the slice: x: 2, y: 2, z: 4, core: 2. Of those that a mesh axis runs over, the one named last changes fastest.
Arguments:
- tile_values: bfloat16 [8, 4, 320, 128, 128], P('rows', 'cols'), may hold values from -0.0625 to 0.0625
- tile_rows: int32 [8, 4, 320], P('rows', 'cols'), may hold values from 0 to 7
- tile_cols: int32 [8, 4, 320], P('rows', 'cols'), may hold values from 0 to 15
- tile_counts: int32 [8, 4], P('rows', 'cols'), may hold values from 1 to 320, as said below
- sketch: bfloat16 [8192, 160], P(('rows', 'cols')), may hold values from -6 to 6
Outputs:
- basis: float32 [8192, 160], P(('rows', 'cols'))
- factor: float32 [160, 160], replicated
The draws below stay inside these ranges and needn't reach their ends.
Inputs may be any that keep to these rules, and one draw needn't show every extreme that they name: Only the first tile_counts[r, c] slots of list (r, c) are live; some list has all 320 slots live in every draw. `tile_cols`: the same place may stand in several live slots of a list.
All inputs are finite; a program needn't handle non-finite values.
Results may differ from the reference program's by a relative error of at most 0.0029.
Values may be sent and summed in bfloat16 or wider, within the bound.
A program may use at most 128 MiB of HBM per device.

```python
import jax
import jax.numpy as jnp
from jax import lax

TILE = 128
SKETCH = 160
POWER = 2
RT = 8
SLOTS = 320
TPD = 2
CT = 16
NODES = 8192
N_ROWS = 8
N_COLS = 4


def draw_tile_counts(key, part):
    first_key, second_key = jax.random.split(key)
    uniform_draw = jax.random.randint(first_key, (N_ROWS * N_COLS,), 0, SLOTS + 1)
    counts_drawn = jnp.maximum(uniform_draw * uniform_draw // SLOTS, 1)
    fullest = jax.random.randint(second_key, (), 0, N_ROWS * N_COLS)
    counts_drawn = jnp.where(jnp.arange(N_ROWS * N_COLS, dtype=jnp.int32) == fullest, SLOTS, counts_drawn)
    return counts_drawn.reshape(N_ROWS, N_COLS).astype(jnp.int32)


def place_ends(drawn, stream_key, smallest, top_value):
    extent = drawn.shape
    place = [jax.random.randint(jax.random.fold_in(stream_key, axis), (), 0, extent[axis]) for axis in range(len(extent))]
    drawn = drawn.at[tuple(place)].set(smallest)
    longest = extent.index(max(extent))
    place[longest] = (place[longest] + 1) % extent[longest]
    return drawn.at[tuple(place)].set(top_value)


def shard_levels(key, dims, cuts, low, largest):
    def one(dim, blocks):
        draws = jax.random.uniform(jax.random.fold_in(jax.random.fold_in(key, 6), dim), (blocks,), jnp.float32, low / len(cuts), largest / len(cuts))
        return jnp.repeat(jnp.exp(draws), dims[dim] // blocks).reshape((-1,) + (1,) * (len(dims) - dim - 1))

    gain = one(*cuts[0])
    for cut in cuts[1:]:
        gain = gain * one(*cut)
    return gain


def centred(stream_key, dims, deviation, bound, shards=(), kind=jnp.bfloat16):
    values = jax.random.normal(stream_key, dims, jnp.float32) * deviation
    if len(shards) > 0:
        values = shard_levels(stream_key, dims, shards, -0.22, 0.18) * values
    return jnp.clip(values, min=-bound, max=bound).astype(kind)


def setup_inputs(seed: int = 0) -> dict:
    streams_of = jax.random.split(jax.random.key(seed), 6)
    tile_values = centred(streams_of[0], (N_ROWS, N_COLS, SLOTS, TILE, TILE), (TILE * SLOTS * N_COLS // (2 * RT)) ** -0.5, 0.0625, ((0, 8), (1, 4)))
    tile_rows = place_ends(jax.random.randint(streams_of[1], (N_ROWS, N_COLS, SLOTS), 0, RT), jax.random.fold_in(streams_of[1], 1), 0, RT - 1).astype(jnp.int32)
    tile_cols = place_ends(jax.random.randint(streams_of[2], (N_ROWS, N_COLS, SLOTS), 0, CT), jax.random.fold_in(streams_of[2], 1), 0, CT - 1).astype(jnp.int32)
    tile_counts = draw_tile_counts(jax.random.fold_in(streams_of[5], 71), 0)
    sketch = centred(streams_of[4], (NODES, SKETCH), 1.0, 6.0, ((0, 32),))
    return dict(tile_values=tile_values, tile_rows=tile_rows, tile_cols=tile_cols, tile_counts=tile_counts, sketch=sketch)


def product(tile_values, tile_rows, tile_cols, tile_counts, current):
    tile_stack = current.reshape(NODES // TILE, TILE, SKETCH)

    def one_list(carry, position):
        row_index = position // N_COLS
        col_index = position % N_COLS
        block_values = tile_values[row_index, col_index].astype(jnp.float32)
        local_tile = tile_cols[row_index, col_index]
        global_tile = (local_tile // TPD * N_COLS + col_index) * TPD + local_tile % TPD
        picked = tile_stack[global_tile.astype(jnp.int32)].astype(jnp.float32)
        products = jnp.einsum('sab,sbk->sak', block_values, picked, precision=lax.Precision.HIGHEST)
        live_mask = (jnp.arange(SLOTS, dtype=jnp.int32) < tile_counts[row_index, col_index]).astype(jnp.float32)
        onehot = (tile_rows[row_index, col_index][None, :] == jnp.arange(RT, dtype=jnp.int32)[:, None]).astype(jnp.float32)
        onehot = onehot * live_mask[None, :]
        row_block = jnp.einsum('rs,sak->rak', onehot, products, precision=lax.Precision.HIGHEST)
        return (carry, row_block.reshape(RT * TILE, SKETCH))
    _, blocks = lax.scan(one_list, None, jnp.arange(N_ROWS * N_COLS, dtype=jnp.int32))
    return blocks.reshape(N_ROWS, N_COLS, RT * TILE, SKETCH).sum(axis=1).reshape(NODES, SKETCH)

def reference(tile_values, tile_rows, tile_cols, tile_counts, sketch):
    current = sketch
    solved = None
    factor = None
    for power in range(POWER):
        image = product(tile_values, tile_rows, tile_cols, tile_counts, current)
        gram_matrix = jnp.dot(image.T, image, precision=lax.Precision.HIGHEST) / NODES
        factor = jnp.linalg.cholesky(gram_matrix)
        solved = lax.linalg.triangular_solve(factor, image, left_side=False, lower=True, transpose_a=True)
        current = solved.astype(jnp.bfloat16)
    return (solved, factor)
```

```python
import functools
import math

import jax
import jax.numpy as jnp
from jax import lax
from jax.experimental import pallas as pl
from jax.experimental.pallas import tpu as pltpu
from jax.sharding import PartitionSpec as P

POWER = 2
RT = 8
LANES = 128
BLOCK = 32
VMEM_BYTES = 60 * 1024 * 1024
MESH = pl.DeviceIdType.MESH
HIGHEST = lax.Precision.HIGHEST
NT = (((1,), (1,)), ((), ()))
TN = (((0,), (0,)), ((), ()))


def densify_kernel(height, pair, rows_ref, cols_ref, count_ref, tiles_ref, high_ref, low_ref, head, size, following):
    groups = high_ref.shape[0]
    tile = tiles_ref.shape[1]
    places = groups * pair * height

    def clear(place, _):
        head[place] = 0
        size[place] = 0
        return 0

    def link(slot, _):
        place = cols_ref[slot] * height + rows_ref[slot]
        following[slot] = head[place]
        head[place] = slot
        size[place] = size[place] + 1
        return 0

    lax.fori_loop(0, places, clear, 0)
    lax.fori_loop(0, count_ref[0], link, 0)

    def one_place(index, _):
        group = index // height
        row = index % height
        for part in range(pair):
            place = (group * pair + part) * height + row

            def add(_, carry):
                slot, total = carry
                return following[slot], total + tiles_ref[slot].astype(jnp.float32)

            start = (head[place], jnp.zeros((tile, tile), jnp.float32))
            _, total = lax.fori_loop(0, size[place], add, start)
            high = total.astype(jnp.bfloat16)
            low = (total - high.astype(jnp.float32)).astype(jnp.bfloat16)
            where = pl.ds(pl.multiple_of(row * tile, tile), tile)
            high_ref[group, where, part * tile:(part + 1) * tile] = high
            low_ref[group, where, part * tile:(part + 1) * tile] = low
        return 0

    lax.fori_loop(0, groups * height, one_place, 0)


def densify(tile_values, tile_rows, tile_cols, tile_counts, groups, pair):
    slots, tile = tile_values.shape[:2]
    places = groups * pair * RT
    smem = pl.BlockSpec(memory_space=pltpu.SMEM)
    vmem = pl.BlockSpec(memory_space=pltpu.VMEM)
    dense = jax.ShapeDtypeStruct((groups, RT * tile, pair * tile), jnp.bfloat16)
    return pl.pallas_call(
        functools.partial(densify_kernel, RT, pair),
        out_shape=(dense, dense),
        in_specs=[smem, smem, smem, vmem],
        out_specs=(vmem, vmem),
        scratch_shapes=[
            pltpu.SMEM((places,), jnp.int32),
            pltpu.SMEM((places,), jnp.int32),
            pltpu.SMEM((slots,), jnp.int32),
        ],
        compiler_params=pltpu.CompilerParams(vmem_limit_bytes=VMEM_BYTES),
        name="densify",
    )(tile_rows, tile_cols, tile_counts, tile_values)


def image_kernel(
    n_rows, n_cols, current_ref, high_ref, low_ref, image_ref, gram_ref,
    gathered, part, came, packed, gram_cols, gram_rows, gram_whole,
    own_send, own_recv, pass_send, pass_recv, part_send, part_recv,
    gc_send, gc_recv, gr_send, gr_recv, gw_send, gw_recv,
):
    row = lax.axis_index("rows")
    col = lax.axis_index("cols")
    width, share = current_ref.shape
    deep = n_rows // 2
    z = row // 2
    y = row % 2
    mate = z * 2 + 1 - y

    def send(src, dst, send_sem, recv_sem, **where):
        return pltpu.make_async_remote_copy(
            src_ref=src, dst_ref=dst, send_sem=send_sem, recv_sem=recv_sem,
            device_id=where, device_id_type=MESH,
        )

    barrier = pltpu.get_barrier_semaphore()
    for step in range(1, n_rows):
        pl.semaphore_signal(barrier, inc=1, device_id={"rows": (row + step) % n_rows}, device_id_type=MESH)
    for step in range(1, n_cols):
        pl.semaphore_signal(barrier, inc=1, device_id={"cols": (col + step) % n_cols}, device_id_type=MESH)
    pl.semaphore_wait(barrier, n_rows + n_cols - 2)

    sent = []
    own = send(current_ref, gathered.at[row], pass_send.at[z], pass_recv.at[z], rows=mate)
    own.start()
    sent.append(own)
    for step in range(1, deep):
        to = ((z + step) % deep) * 2 + y
        copy = send(current_ref, gathered.at[row], own_send.at[step], own_recv.at[z], rows=to)
        copy.start()
        sent.append(copy)

    def multiply(value, source, first):
        for piece in range(n_cols):
            high = high_ref[source, piece * share:(piece + 1) * share, :]
            low = low_ref[source, piece * share:(piece + 1) * share, :]
            got = lax.dot_general(value, high, NT, preferred_element_type=jnp.float32)
            got = got + lax.dot_general(value, low, NT, preferred_element_type=jnp.float32)
            part[piece] = got if first else part[piece] + got

    multiply(current_ref[...], row, True)
    for step in range(1, deep):
        other = (z + step) % deep
        source = other * 2 + y
        send(current_ref, gathered.at[source], own_send.at[step], own_recv.at[other], rows=mate).wait_recv()
        copy = send(gathered.at[source], gathered.at[source], pass_send.at[other], pass_recv.at[other], rows=mate)
        copy.start()
        sent.append(copy)
        multiply(gathered[source], source, False)
    for step in range(deep):
        other = (z + step) % deep
        source = other * 2 + 1 - y
        send(current_ref, gathered.at[source], pass_send.at[other], pass_recv.at[other], rows=mate).wait_recv()
        multiply(gathered[source], source, False)
    for copy in sent:
        copy.wait_send()

    twin = col + 1 - 2 * (col % 2)
    across = (col + 2) % 4
    twin_across = (twin + 2) % 4
    first = send(part.at[twin_across], came.at[1], part_send.at[1], part_recv.at[1], cols=twin)
    second = send(part.at[twin], came.at[0], part_send.at[0], part_recv.at[0], cols=twin)
    first.start()
    second.start()
    first.wait()
    came[3] = part[across] + came[1]
    third = send(came.at[3], came.at[2], part_send.at[2], part_recv.at[2], cols=across)
    third.start()
    second.wait()
    near = part[col] + came[0]
    third.wait()
    image = near + came[2]
    image_ref[...] = image

    gram = lax.dot_general(image, image, NT, precision=HIGHEST, preferred_element_type=jnp.float32)
    rest = width - LANES
    packed[0:width, :] = gram[:, 0:LANES]
    packed[width:width + rest, :] = jnp.zeros((rest, LANES), jnp.float32)
    packed[width:width + rest, 0:rest] = gram[LANES:width, LANES:width]
    piece_rows = (width + rest) // n_cols
    copies = []
    for step in range(1, n_cols):
        to = (col + step) % n_cols
        src = packed.at[pl.ds(pl.multiple_of(to * piece_rows, 8), piece_rows)]
        copy = send(src, gram_cols.at[col], gc_send.at[step], gc_recv.at[col], cols=to)
        copy.start()
        copies.append(copy)
    gram_cols[col] = packed[pl.ds(pl.multiple_of(col * piece_rows, 8), piece_rows), :]
    for step in range(1, n_cols):
        source = (col + step) % n_cols
        send(packed.at[pl.ds(0, piece_rows)], gram_cols.at[source], gc_send.at[step], gc_recv.at[source], cols=source).wait_recv()
    total = gram_cols[0]
    for piece in range(1, n_cols):
        total = total + gram_cols[piece]
    gram_rows[row] = total
    for step in range(1, n_rows):
        to = (row + step) % n_rows
        copy = send(gram_rows.at[row], gram_rows.at[row], gr_send.at[step], gr_recv.at[row], rows=to)
        copy.start()
        copies.append(copy)
    for step in range(1, n_rows):
        source = (row + step) % n_rows
        send(gram_rows.at[source], gram_rows.at[source], gr_send.at[step], gr_recv.at[source], rows=source).wait_recv()
    total = gram_rows[0]
    for piece in range(1, n_rows):
        total = total + gram_rows[piece]
    gram_whole[col] = total
    for step in range(1, n_cols):
        to = (col + step) % n_cols
        copy = send(gram_whole.at[col], gram_whole.at[col], gw_send.at[step], gw_recv.at[col], cols=to)
        copy.start()
        copies.append(copy)
    for step in range(1, n_cols):
        source = (col + step) % n_cols
        send(gram_whole.at[source], gram_whole.at[source], gw_send.at[step], gw_recv.at[source], cols=source).wait_recv()
    for piece in range(n_cols):
        gram_ref[piece * piece_rows:(piece + 1) * piece_rows, :] = gram_whole[piece]
    for copy in copies:
        copy.wait_send()


def image_step(n_rows, n_cols, current, high, low):
    width, share = current.shape
    lines = 2 * width - LANES
    piece = lines // n_cols
    vmem = pl.BlockSpec(memory_space=pltpu.VMEM)
    dma = pltpu.SemaphoreType.DMA
    f32 = jnp.float32
    return pl.pallas_call(
        functools.partial(image_kernel, n_rows, n_cols),
        out_shape=(jax.ShapeDtypeStruct((width, share), f32), jax.ShapeDtypeStruct((lines, LANES), f32)),
        in_specs=[vmem, vmem, vmem],
        out_specs=(vmem, vmem),
        scratch_shapes=[
            pltpu.VMEM((n_rows, width, share), jnp.bfloat16),
            pltpu.VMEM((n_cols, width, share), f32),
            pltpu.VMEM((4, width, share), f32),
            pltpu.VMEM((lines, LANES), f32),
            pltpu.VMEM((n_cols, piece, LANES), f32),
            pltpu.VMEM((n_rows, piece, LANES), f32),
            pltpu.VMEM((n_cols, piece, LANES), f32),
            dma((n_rows // 2,)), dma((n_rows // 2,)), dma((n_rows // 2,)), dma((n_rows // 2,)),
            dma((3,)), dma((3,)),
            dma((n_cols,)), dma((n_cols,)), dma((n_rows,)), dma((n_rows,)), dma((n_cols,)), dma((n_cols,)),
        ],
        compiler_params=pltpu.CompilerParams(
            collective_id=0, has_side_effects=True, vmem_limit_bytes=VMEM_BYTES
        ),
        name="image_step",
    )(current, high, low)


def solve_kernel(nodes, packed_ref, image_ref, solved_ref, rounded_ref, upper_ref, work):
    width = image_ref.shape[0]
    rest = width - LANES
    half = work.shape[1] // 2
    work[...] = jnp.zeros_like(work)
    work[:, 0:LANES] = packed_ref[0:width, :] / nodes
    work[0:LANES, LANES:width] = (packed_ref[LANES:width, :] / nodes).T
    work[LANES:width, LANES:width] = packed_ref[width:width + rest, 0:rest] / nodes
    row_ids = lax.broadcasted_iota(jnp.int32, (width, half), 0)
    col_ids = lax.broadcasted_iota(jnp.int32, (width, half), 1)
    work[:, half:] = (row_ids == col_ids).astype(jnp.float32)
    r_ids = lax.broadcasted_iota(jnp.int32, (BLOCK, BLOCK), 0)
    c_ids = lax.broadcasted_iota(jnp.int32, (BLOCK, BLOCK), 1)
    eye = r_ids == c_ids
    lines = lax.broadcasted_iota(jnp.int32, (BLOCK, 1), 0)
    for first in range(0, width, BLOCK):
        last = first + BLOCK
        diag = work[first:last, first:last]
        inverse = eye.astype(jnp.float32)
        for j in range(BLOCK):
            scale = jnp.where(lines > j, diag[:, j:j + 1] / diag[j:j + 1, j:j + 1], 0.0)
            inverse = inverse - scale * inverse[j:j + 1, :]
            diag = diag - scale * diag[j:j + 1, :]
        pivots = jnp.sum(jnp.where(eye, diag, 0.0), axis=1, keepdims=True)
        inverse = inverse / jnp.sqrt(pivots)
        panel = jnp.dot(inverse, work[first:last, :], precision=HIGHEST, preferred_element_type=jnp.float32)
        work[first:last, :] = panel
        if last < width:
            drop = lax.dot_general(panel[:, last:width], panel, TN, precision=HIGHEST, preferred_element_type=jnp.float32)
            work[last:width, :] = work[last:width, :] - drop
    upper_ref[...] = jnp.where(col_ids >= row_ids, work[:, 0:half], 0.0)[:, 0:width]
    solved = jnp.dot(work[:, half:half + width], image_ref[...], precision=HIGHEST, preferred_element_type=jnp.float32)
    solved_ref[...] = solved
    rounded_ref[...] = solved.astype(jnp.bfloat16)


def solve_step(nodes, packed, image):
    width, share = image.shape
    vmem = pl.BlockSpec(memory_space=pltpu.VMEM)
    return pl.pallas_call(
        functools.partial(solve_kernel, nodes),
        out_shape=(
            jax.ShapeDtypeStruct((width, share), jnp.float32),
            jax.ShapeDtypeStruct((width, share), jnp.bfloat16),
            jax.ShapeDtypeStruct((width, width), jnp.float32),
        ),
        in_specs=[vmem, vmem],
        out_specs=(vmem, vmem, vmem),
        scratch_shapes=[pltpu.VMEM((width, 4 * LANES), jnp.float32)],
        compiler_params=pltpu.CompilerParams(vmem_limit_bytes=VMEM_BYTES),
        name="solve_step",
    )(packed, image)


def dense_shards(n_rows, n_cols, tile_values, tile_rows, tile_cols, tile_counts, sketch):
    tile = tile_values.shape[-1]
    pair = sketch.shape[0] // tile
    high, low = densify(tile_values[0, 0], tile_rows[0, 0], tile_cols[0, 0], tile_counts[0], n_rows, pair)
    current = sketch.T
    nodes = float(sketch.shape[0] * n_rows * n_cols)
    for power in range(POWER):
        image, packed = image_step(n_rows, n_cols, current, high, low)
        solved, current, upper = solve_step(nodes, packed, image)
    return (solved.T, upper.T)


def fits_dense(mesh, tile_values, sketch):
    n_rows, n_cols = mesh.shape["rows"], mesh.shape["cols"]
    tile = tile_values.shape[-1]
    share = sketch.shape[0] // (n_rows * n_cols)
    width = sketch.shape[1]
    dense = n_rows * share * RT * tile * 2
    lists = tile_values.shape[2] * tile * tile * 2
    return (
        n_cols == 4 and n_rows % 2 == 0 and tile == LANES and share % tile == 0
        and RT * tile == n_cols * share and LANES < width <= 2 * LANES and width % BLOCK == 0
        and (2 * width - LANES) % (8 * n_cols) == 0 and 2 * dense + lists < 40 * 1024 * 1024
    )


def accumulate(block_list, row_list, col_list, live_count, gathered, height):
    slot_total = block_list.shape[0]
    tile_size = block_list.shape[1]
    sketch_width = gathered.shape[1]
    tile_stack = gathered.reshape(-1, tile_size, sketch_width)
    block_size = math.gcd(32, slot_total)

    def one_block(block_index, running):
        first_slot = block_index * block_size
        block_values = lax.dynamic_slice_in_dim(block_list, first_slot, block_size, 0)
        rowids = lax.dynamic_slice_in_dim(row_list, first_slot, block_size, 0)
        colids = lax.dynamic_slice_in_dim(col_list, first_slot, block_size, 0)
        picked = jnp.take(tile_stack, colids, axis=0)
        products = jnp.einsum(
            "sab,sbk->sak", block_values, picked, preferred_element_type=jnp.float32
        )
        live_mask = (first_slot + jnp.arange(block_size, dtype=jnp.int32) < live_count).astype(
            jnp.float32
        )
        return running.at[rowids].add(products * live_mask[:, None, None])

    block_count = (live_count + block_size - 1) // block_size
    initial = jnp.zeros((height, tile_size, sketch_width), jnp.float32)
    running = lax.fori_loop(0, block_count, one_block, initial)
    return running.reshape(height * tile_size, sketch_width)


def shards(tile_values, tile_rows, tile_cols, tile_counts, sketch):
    own_values = tile_values[0, 0]
    own_rows = tile_rows[0, 0]
    own_cols = tile_cols[0, 0]
    own_count = tile_counts[0, 0]
    nodes_total = sketch.shape[0] * lax.axis_size("rows") * lax.axis_size("cols")
    current = sketch
    solved = None
    factor = None
    for power in range(POWER):
        gathered = lax.all_gather(current, "rows", axis=0, tiled=True)
        partial_value = accumulate(own_values, own_rows, own_cols, own_count, gathered, RT)
        whole = lax.psum(partial_value, "cols")
        gram_matrix = lax.psum(jnp.dot(whole.T, whole, precision=lax.Precision.HIGHEST), "rows")
        share_rows = whole.shape[0] // lax.axis_size("cols")
        owned = lax.dynamic_slice_in_dim(whole, lax.axis_index("cols") * share_rows, share_rows, 0)
        gram_matrix = gram_matrix / nodes_total
        factor = jnp.linalg.cholesky(gram_matrix)
        solved = lax.linalg.triangular_solve(
            factor, owned, left_side=False, lower=True, transpose_a=True
        )
        current = solved.astype(jnp.bfloat16)
    return (solved, factor)


def solution(mesh):
    placed = (
        P("rows", "cols", None, None, None),
        P("rows", "cols", None),
        P("rows", "cols", None),
        P("rows", "cols"),
        P(("rows", "cols"), None),
    )

    def run(*arrays):
        body = shards
        if fits_dense(mesh, arrays[0], arrays[4]):
            body = functools.partial(dense_shards, mesh.shape["rows"], mesh.shape["cols"])
        return jax.shard_map(
            body,
            mesh=mesh,
            in_specs=placed,
            out_specs=(P(("rows", "cols"), None), P()),
            check_vma=False,
        )(*arrays)

    return run
```

```python
import functools
import math

import jax
import jax.numpy as jnp
from jax import lax
from jax.experimental import pallas as pl
from jax.experimental.pallas import tpu as pltpu
from jax.sharding import PartitionSpec as P

POWER = 2
RT = 8
LANES = 128
BLOCK = 32
VMEM_BYTES = 60 * 1024 * 1024
MESH = pl.DeviceIdType.MESH
HIGHEST = lax.Precision.HIGHEST
NT = (((1,), (1,)), ((), ()))
TN = (((0,), (0,)), ((), ()))


def densify_kernel(
    height, pair, rows_ref, cols_ref, count_ref, values_ref, high_ref, low_ref,
    tiles_ref, head, size, following, loaded,
):
    groups = high_ref.shape[0]
    tile = tiles_ref.shape[1]
    places = groups * pair * height
    load = pltpu.make_async_copy(values_ref, tiles_ref, loaded)
    load.start()

    def clear(place, _):
        head[place] = 0
        size[place] = 0
        return 0

    def link(slot, _):
        place = cols_ref[0, 0, slot] * height + rows_ref[0, 0, slot]
        following[slot] = head[place]
        head[place] = slot
        size[place] = size[place] + 1
        return 0

    lax.fori_loop(0, places, clear, 0)
    lax.fori_loop(0, count_ref[0, 0], link, 0)
    load.wait()

    def one_place(index, _):
        group = index // height
        row = index % height
        for part in range(pair):
            place = (group * pair + part) * height + row

            def add(_, carry):
                slot, total = carry
                return following[slot], total + tiles_ref[slot].astype(jnp.float32)

            start = (head[place], jnp.zeros((tile, tile), jnp.float32))
            _, total = lax.fori_loop(0, size[place], add, start)
            high = total.astype(jnp.bfloat16)
            low = (total - high.astype(jnp.float32)).astype(jnp.bfloat16)
            where = pl.ds(pl.multiple_of(row * tile, tile), tile)
            high_ref[group, where, part * tile:(part + 1) * tile] = high
            low_ref[group, where, part * tile:(part + 1) * tile] = low
        return 0

    lax.fori_loop(0, groups * height, one_place, 0)


def densify(tile_values, tile_rows, tile_cols, tile_counts, groups, pair):
    slots, tile = tile_values.shape[:2]
    places = groups * pair * RT
    smem = pl.BlockSpec(memory_space=pltpu.SMEM)
    vmem = pl.BlockSpec(memory_space=pltpu.VMEM)
    dense = jax.ShapeDtypeStruct((groups, RT * tile, pair * tile), jnp.bfloat16)
    return pl.pallas_call(
        functools.partial(densify_kernel, RT, pair),
        out_shape=(dense, dense),
        in_specs=[smem, smem, smem, pl.BlockSpec(memory_space=pl.ANY)],
        out_specs=(vmem, vmem),
        scratch_shapes=[
            pltpu.VMEM(tile_values.shape, tile_values.dtype),
            pltpu.SMEM((places,), jnp.int32),
            pltpu.SMEM((places,), jnp.int32),
            pltpu.SMEM((slots,), jnp.int32),
            pltpu.SemaphoreType.DMA,
        ],
        compiler_params=pltpu.CompilerParams(vmem_limit_bytes=VMEM_BYTES),
        name="densify",
    )(tile_rows, tile_cols, tile_counts, tile_values)


def image_kernel(
    n_rows, n_cols, current_ref, high_hbm, low_hbm, image_ref, gram_ref,
    high_ref, low_ref, loaded, gathered, part, came, packed, gram_cols, gram_rows, gram_whole,
    own_send, own_recv, pass_send, pass_recv, part_send, part_recv,
    gc_send, gc_recv, gr_send, gr_recv, gw_send, gw_recv,
):
    row = lax.axis_index("rows")
    col = lax.axis_index("cols")
    width, share = current_ref.shape
    deep = n_rows // 2
    z = row // 2
    y = row % 2
    mate = z * 2 + 1 - y

    def send(src, dst, send_sem, recv_sem, **where):
        return pltpu.make_async_remote_copy(
            src_ref=src, dst_ref=dst, send_sem=send_sem, recv_sem=recv_sem,
            device_id=where, device_id_type=MESH,
        )

    loads = [
        pltpu.make_async_copy(high_hbm, high_ref, loaded.at[0]),
        pltpu.make_async_copy(low_hbm, low_ref, loaded.at[1]),
    ]
    for load in loads:
        load.start()
    barrier = pltpu.get_barrier_semaphore()
    for step in range(1, n_rows):
        pl.semaphore_signal(barrier, inc=1, device_id={"rows": (row + step) % n_rows}, device_id_type=MESH)
    for step in range(1, n_cols):
        pl.semaphore_signal(barrier, inc=1, device_id={"cols": (col + step) % n_cols}, device_id_type=MESH)
    pl.semaphore_wait(barrier, n_rows + n_cols - 2)

    sent = []
    own = send(current_ref, gathered.at[row], pass_send.at[z], pass_recv.at[z], rows=mate)
    own.start()
    sent.append(own)
    for step in range(1, deep):
        to = ((z + step) % deep) * 2 + y
        copy = send(current_ref, gathered.at[row], own_send.at[step], own_recv.at[z], rows=to)
        copy.start()
        sent.append(copy)

    def multiply(value, source, first):
        for piece in range(n_cols):
            high = high_ref[source, piece * share:(piece + 1) * share, :]
            low = low_ref[source, piece * share:(piece + 1) * share, :]
            got = lax.dot_general(value, high, NT, preferred_element_type=jnp.float32)
            got = got + lax.dot_general(value, low, NT, preferred_element_type=jnp.float32)
            part[piece] = got if first else part[piece] + got

    for load in loads:
        load.wait()
    multiply(current_ref[...], row, True)
    for step in range(1, deep):
        other = (z + step) % deep
        source = other * 2 + y
        send(current_ref, gathered.at[source], own_send.at[step], own_recv.at[other], rows=mate).wait_recv()
        copy = send(gathered.at[source], gathered.at[source], pass_send.at[other], pass_recv.at[other], rows=mate)
        copy.start()
        sent.append(copy)
        multiply(gathered[source], source, False)
    for step in range(deep):
        other = (z + step) % deep
        source = other * 2 + 1 - y
        send(current_ref, gathered.at[source], pass_send.at[other], pass_recv.at[other], rows=mate).wait_recv()
        multiply(gathered[source], source, False)
    for copy in sent:
        copy.wait_send()

    twin = col + 1 - 2 * (col % 2)
    across = (col + 2) % 4
    twin_across = (twin + 2) % 4
    first = send(part.at[twin_across], came.at[1], part_send.at[1], part_recv.at[1], cols=twin)
    second = send(part.at[twin], came.at[0], part_send.at[0], part_recv.at[0], cols=twin)
    first.start()
    second.start()
    first.wait()
    came[3] = part[across] + came[1]
    third = send(came.at[3], came.at[2], part_send.at[2], part_recv.at[2], cols=across)
    third.start()
    second.wait()
    near = part[col] + came[0]
    third.wait()
    image = near + came[2]
    image_ref[...] = image

    gram = lax.dot_general(image, image, NT, precision=HIGHEST, preferred_element_type=jnp.float32)
    rest = width - LANES
    packed[0:width, :] = gram[:, 0:LANES]
    packed[width:width + rest, :] = jnp.zeros((rest, LANES), jnp.float32)
    packed[width:width + rest, 0:rest] = gram[LANES:width, LANES:width]
    piece_rows = (width + rest) // n_cols
    copies = []
    for step in range(1, n_cols):
        to = (col + step) % n_cols
        src = packed.at[pl.ds(pl.multiple_of(to * piece_rows, 8), piece_rows)]
        copy = send(src, gram_cols.at[col], gc_send.at[step], gc_recv.at[col], cols=to)
        copy.start()
        copies.append(copy)
    gram_cols[col] = packed[pl.ds(pl.multiple_of(col * piece_rows, 8), piece_rows), :]
    for step in range(1, n_cols):
        source = (col + step) % n_cols
        send(packed.at[pl.ds(0, piece_rows)], gram_cols.at[source], gc_send.at[step], gc_recv.at[source], cols=source).wait_recv()
    total = gram_cols[0]
    for piece in range(1, n_cols):
        total = total + gram_cols[piece]
    gram_rows[row] = total
    for step in range(1, n_rows):
        to = (row + step) % n_rows
        copy = send(gram_rows.at[row], gram_rows.at[row], gr_send.at[step], gr_recv.at[row], rows=to)
        copy.start()
        copies.append(copy)
    for step in range(1, n_rows):
        source = (row + step) % n_rows
        send(gram_rows.at[source], gram_rows.at[source], gr_send.at[step], gr_recv.at[source], rows=source).wait_recv()
    total = gram_rows[0]
    for piece in range(1, n_rows):
        total = total + gram_rows[piece]
    gram_whole[col] = total
    for step in range(1, n_cols):
        to = (col + step) % n_cols
        copy = send(gram_whole.at[col], gram_whole.at[col], gw_send.at[step], gw_recv.at[col], cols=to)
        copy.start()
        copies.append(copy)
    for step in range(1, n_cols):
        source = (col + step) % n_cols
        send(gram_whole.at[source], gram_whole.at[source], gw_send.at[step], gw_recv.at[source], cols=source).wait_recv()
    for piece in range(n_cols):
        gram_ref[piece * piece_rows:(piece + 1) * piece_rows, :] = gram_whole[piece]
    for copy in copies:
        copy.wait_send()


def image_step(n_rows, n_cols, current, high, low):
    width, share = current.shape
    lines = 2 * width - LANES
    piece = lines // n_cols
    vmem = pl.BlockSpec(memory_space=pltpu.VMEM)
    dma = pltpu.SemaphoreType.DMA
    f32 = jnp.float32
    return pl.pallas_call(
        functools.partial(image_kernel, n_rows, n_cols),
        out_shape=(jax.ShapeDtypeStruct((width, share), f32), jax.ShapeDtypeStruct((lines, LANES), f32)),
        in_specs=[vmem, pl.BlockSpec(memory_space=pl.ANY), pl.BlockSpec(memory_space=pl.ANY)],
        out_specs=(vmem, vmem),
        scratch_shapes=[
            pltpu.VMEM(high.shape, high.dtype),
            pltpu.VMEM(low.shape, low.dtype),
            dma((2,)),
            pltpu.VMEM((n_rows, width, share), jnp.bfloat16),
            pltpu.VMEM((n_cols, width, share), f32),
            pltpu.VMEM((4, width, share), f32),
            pltpu.VMEM((lines, LANES), f32),
            pltpu.VMEM((n_cols, piece, LANES), f32),
            pltpu.VMEM((n_rows, piece, LANES), f32),
            pltpu.VMEM((n_cols, piece, LANES), f32),
            dma((n_rows // 2,)), dma((n_rows // 2,)), dma((n_rows // 2,)), dma((n_rows // 2,)),
            dma((3,)), dma((3,)),
            dma((n_cols,)), dma((n_cols,)), dma((n_rows,)), dma((n_rows,)), dma((n_cols,)), dma((n_cols,)),
        ],
        compiler_params=pltpu.CompilerParams(
            collective_id=0, has_side_effects=True, vmem_limit_bytes=VMEM_BYTES
        ),
        name="image_step",
    )(current, high, low)


def solve_kernel(nodes, packed_ref, image_ref, solved_ref, rounded_ref, factor_ref, work):
    width = image_ref.shape[0]
    rest = width - LANES
    half = work.shape[1] // 2
    work[...] = jnp.zeros_like(work)
    work[:, 0:LANES] = packed_ref[0:width, :] / nodes
    work[0:LANES, LANES:width] = (packed_ref[LANES:width, :] / nodes).T
    work[LANES:width, LANES:width] = packed_ref[width:width + rest, 0:rest] / nodes
    row_ids = lax.broadcasted_iota(jnp.int32, (width, half), 0)
    col_ids = lax.broadcasted_iota(jnp.int32, (width, half), 1)
    work[:, half:] = (row_ids == col_ids).astype(jnp.float32)
    r_ids = lax.broadcasted_iota(jnp.int32, (BLOCK, BLOCK), 0)
    c_ids = lax.broadcasted_iota(jnp.int32, (BLOCK, BLOCK), 1)
    eye = r_ids == c_ids
    lines = lax.broadcasted_iota(jnp.int32, (BLOCK, 1), 0)
    for first in range(0, width, BLOCK):
        last = first + BLOCK
        diag = work[first:last, first:last]
        inverse = eye.astype(jnp.float32)
        for j in range(0, BLOCK, 2):
            one = jnp.broadcast_to(diag[:, j:j + 1], (BLOCK, BLOCK))
            two = jnp.broadcast_to(diag[:, j + 1:j + 2], (BLOCK, BLOCK))
            a, b, c = one[j:j + 1, :], one[j + 1:j + 2, :], two[j + 1:j + 2, :]
            u, v = diag[j:j + 1, :], diag[j + 1:j + 2, :]
            s, t = inverse[j:j + 1, :], inverse[j + 1:j + 2, :]
            slope = b * (1.0 / a)
            below = lines > j + 1
            left = jnp.where(below, one, 0.0)
            right = jnp.where(below, two, 0.0) - left * slope
            v_low, t_low = v - slope * u, t - slope * s
            first_scale, second_scale = 1.0 / a, 1.0 / (c - slope * b)
            diag = diag - left * (u * first_scale) - right * (v_low * second_scale)
            inverse = inverse - left * (s * first_scale) - right * (t_low * second_scale)
            diag = jnp.where(lines == j + 1, v_low, diag)
            inverse = jnp.where(lines == j + 1, t_low, inverse)
        pivots = jnp.sum(jnp.where(eye, diag, 0.0), axis=1, keepdims=True)
        inverse = inverse / jnp.sqrt(pivots)
        panel = jnp.dot(inverse, work[first:last, :], precision=HIGHEST, preferred_element_type=jnp.float32)
        work[first:last, :] = panel
        if last < width:
            drop = lax.dot_general(panel[:, last:width], panel, TN, precision=HIGHEST, preferred_element_type=jnp.float32)
            work[last:width, :] = work[last:width, :] - drop
    factor = jnp.where(col_ids >= row_ids, work[:, 0:half], 0.0).T
    factor_ref[...] = factor[0:width, :]
    solved = jnp.dot(work[:, half:half + width], image_ref[...], precision=HIGHEST, preferred_element_type=jnp.float32)
    solved_ref[...] = solved
    rounded_ref[...] = solved.astype(jnp.bfloat16)


def solve_step(nodes, packed, image):
    width, share = image.shape
    vmem = pl.BlockSpec(memory_space=pltpu.VMEM)
    return pl.pallas_call(
        functools.partial(solve_kernel, nodes),
        out_shape=(
            jax.ShapeDtypeStruct((width, share), jnp.float32),
            jax.ShapeDtypeStruct((width, share), jnp.bfloat16),
            jax.ShapeDtypeStruct((width, width), jnp.float32),
        ),
        in_specs=[vmem, vmem],
        out_specs=(vmem, vmem, vmem),
        scratch_shapes=[pltpu.VMEM((width, 4 * LANES), jnp.float32)],
        compiler_params=pltpu.CompilerParams(vmem_limit_bytes=VMEM_BYTES),
        name="solve_step",
    )(packed, image)


def dense_shards(n_rows, n_cols, tile_values, tile_rows, tile_cols, tile_counts, sketch):
    tile = tile_values.shape[-1]
    pair = sketch.shape[0] // tile
    high, low = densify(tile_values[0, 0], tile_rows, tile_cols, tile_counts, n_rows, pair)
    current = sketch.T
    nodes = float(sketch.shape[0] * n_rows * n_cols)
    for power in range(POWER):
        image, packed = image_step(n_rows, n_cols, current, high, low)
        solved, current, factor = solve_step(nodes, packed, image)
    return (solved.T, factor)


def fits_dense(mesh, tile_values, sketch):
    n_rows, n_cols = mesh.shape["rows"], mesh.shape["cols"]
    tile = tile_values.shape[-1]
    share = sketch.shape[0] // (n_rows * n_cols)
    width = sketch.shape[1]
    dense = n_rows * share * RT * tile * 2
    lists = tile_values.shape[2] * tile * tile * 2
    return (
        n_cols == 4 and n_rows % 2 == 0 and tile == LANES and share % tile == 0
        and RT * tile == n_cols * share and LANES < width <= 2 * LANES and width % BLOCK == 0
        and (2 * width - LANES) % (8 * n_cols) == 0 and 2 * dense + lists < 40 * 1024 * 1024
    )


def accumulate(block_list, row_list, col_list, live_count, gathered, height):
    slot_total = block_list.shape[0]
    tile_size = block_list.shape[1]
    sketch_width = gathered.shape[1]
    tile_stack = gathered.reshape(-1, tile_size, sketch_width)
    block_size = math.gcd(32, slot_total)

    def one_block(block_index, running):
        first_slot = block_index * block_size
        block_values = lax.dynamic_slice_in_dim(block_list, first_slot, block_size, 0)
        rowids = lax.dynamic_slice_in_dim(row_list, first_slot, block_size, 0)
        colids = lax.dynamic_slice_in_dim(col_list, first_slot, block_size, 0)
        picked = jnp.take(tile_stack, colids, axis=0)
        products = jnp.einsum(
            "sab,sbk->sak", block_values, picked, preferred_element_type=jnp.float32
        )
        live_mask = (first_slot + jnp.arange(block_size, dtype=jnp.int32) < live_count).astype(
            jnp.float32
        )
        return running.at[rowids].add(products * live_mask[:, None, None])

    block_count = (live_count + block_size - 1) // block_size
    initial = jnp.zeros((height, tile_size, sketch_width), jnp.float32)
    running = lax.fori_loop(0, block_count, one_block, initial)
    return running.reshape(height * tile_size, sketch_width)


def shards(tile_values, tile_rows, tile_cols, tile_counts, sketch):
    own_values = tile_values[0, 0]
    own_rows = tile_rows[0, 0]
    own_cols = tile_cols[0, 0]
    own_count = tile_counts[0, 0]
    nodes_total = sketch.shape[0] * lax.axis_size("rows") * lax.axis_size("cols")
    current = sketch
    solved = None
    factor = None
    for power in range(POWER):
        gathered = lax.all_gather(current, "rows", axis=0, tiled=True)
        partial_value = accumulate(own_values, own_rows, own_cols, own_count, gathered, RT)
        whole = lax.psum(partial_value, "cols")
        gram_matrix = lax.psum(jnp.dot(whole.T, whole, precision=lax.Precision.HIGHEST), "rows")
        share_rows = whole.shape[0] // lax.axis_size("cols")
        owned = lax.dynamic_slice_in_dim(whole, lax.axis_index("cols") * share_rows, share_rows, 0)
        gram_matrix = gram_matrix / nodes_total
        factor = jnp.linalg.cholesky(gram_matrix)
        solved = lax.linalg.triangular_solve(
            factor, owned, left_side=False, lower=True, transpose_a=True
        )
        current = solved.astype(jnp.bfloat16)
    return (solved, factor)


def solution(mesh):
    placed = (
        P("rows", "cols", None, None, None),
        P("rows", "cols", None),
        P("rows", "cols", None),
        P("rows", "cols"),
        P(("rows", "cols"), None),
    )

    def run(*arrays):
        body = shards
        if fits_dense(mesh, arrays[0], arrays[4]):
            body = functools.partial(dense_shards, mesh.shape["rows"], mesh.shape["cols"])
        return jax.shard_map(
            body,
            mesh=mesh,
            in_specs=placed,
            out_specs=(P(("rows", "cols"), None), P()),
            check_vma=False,
        )(*arrays)

    return run
```

```python
import functools
import math

import jax
import jax.numpy as jnp
from jax import lax
from jax.experimental import pallas as pl
from jax.experimental.pallas import tpu as pltpu
from jax.sharding import PartitionSpec as P

POWER = 2
RT = 8
LANES = 128
BLOCK = 32
VMEM_BYTES = 60 * 1024 * 1024
MESH = pl.DeviceIdType.MESH
HIGHEST = lax.Precision.HIGHEST
NT = (((1,), (1,)), ((), ()))
TN = (((0,), (0,)), ((), ()))


def densify_kernel(
    height, pair, rows_ref, cols_ref, count_ref, values_ref, high_ref, low_ref,
    tiles_ref, head, size, following, loaded,
):
    groups = high_ref.shape[0]
    tile = tiles_ref.shape[1]
    places = groups * pair * height
    load = pltpu.make_async_copy(values_ref, tiles_ref, loaded)
    load.start()

    def clear(place, _):
        head[place] = 0
        size[place] = 0
        return 0

    def link(slot, _):
        place = cols_ref[0, 0, slot] * height + rows_ref[0, 0, slot]
        following[slot] = head[place]
        head[place] = slot
        size[place] = size[place] + 1
        return 0

    lax.fori_loop(0, places, clear, 0)
    lax.fori_loop(0, count_ref[0, 0], link, 0)
    load.wait()

    def one_place(index, _):
        group = index // height
        row = index % height
        for part in range(pair):
            place = (group * pair + part) * height + row

            def add(_, carry):
                slot, total = carry
                return following[slot], total + tiles_ref[slot].astype(jnp.float32)

            start = (head[place], jnp.zeros((tile, tile), jnp.float32))
            _, total = lax.fori_loop(0, size[place], add, start)
            high = total.astype(jnp.bfloat16)
            low = (total - high.astype(jnp.float32)).astype(jnp.bfloat16)
            where = pl.ds(pl.multiple_of(row * tile, tile), tile)
            high_ref[group, where, part * tile:(part + 1) * tile] = high
            low_ref[group, where, part * tile:(part + 1) * tile] = low
        return 0

    lax.fori_loop(0, groups * height, one_place, 0)


def densify(tile_values, tile_rows, tile_cols, tile_counts, groups, pair):
    slots, tile = tile_values.shape[:2]
    places = groups * pair * RT
    smem = pl.BlockSpec(memory_space=pltpu.SMEM)
    vmem = pl.BlockSpec(memory_space=pltpu.VMEM)
    dense = jax.ShapeDtypeStruct((groups, RT * tile, pair * tile), jnp.bfloat16)
    return pl.pallas_call(
        functools.partial(densify_kernel, RT, pair),
        out_shape=(dense, dense),
        in_specs=[smem, smem, smem, pl.BlockSpec(memory_space=pl.ANY)],
        out_specs=(vmem, vmem),
        scratch_shapes=[
            pltpu.VMEM(tile_values.shape, tile_values.dtype),
            pltpu.SMEM((places,), jnp.int32),
            pltpu.SMEM((places,), jnp.int32),
            pltpu.SMEM((slots,), jnp.int32),
            pltpu.SemaphoreType.DMA,
        ],
        compiler_params=pltpu.CompilerParams(vmem_limit_bytes=VMEM_BYTES),
        name="densify",
    )(tile_rows, tile_cols, tile_counts, tile_values)


def image_kernel(
    n_rows, n_cols, current_ref, high_hbm, low_hbm, image_ref, gram_ref,
    high_ref, low_ref, loaded, gathered, part, came, packed, gram_cols, gram_rows, gram_whole,
    own_send, own_recv, pass_send, pass_recv, part_send, part_recv,
    gc_send, gc_recv, gr_send, gr_recv, gw_send, gw_recv,
):
    row = lax.axis_index("rows")
    col = lax.axis_index("cols")
    width, share = current_ref.shape
    deep = n_rows // 2
    z = row // 2
    y = row % 2
    mate = z * 2 + 1 - y

    def send(src, dst, send_sem, recv_sem, **where):
        return pltpu.make_async_remote_copy(
            src_ref=src, dst_ref=dst, send_sem=send_sem, recv_sem=recv_sem,
            device_id=where, device_id_type=MESH,
        )

    loads = [
        pltpu.make_async_copy(high_hbm, high_ref, loaded.at[0]),
        pltpu.make_async_copy(low_hbm, low_ref, loaded.at[1]),
    ]
    for load in loads:
        load.start()
    barrier = pltpu.get_barrier_semaphore()
    for step in range(1, n_rows):
        pl.semaphore_signal(barrier, inc=1, device_id={"rows": (row + step) % n_rows}, device_id_type=MESH)
    for step in range(1, n_cols):
        pl.semaphore_signal(barrier, inc=1, device_id={"cols": (col + step) % n_cols}, device_id_type=MESH)
    pl.semaphore_wait(barrier, n_rows + n_cols - 2)

    sent = []
    own = send(current_ref, gathered.at[row], pass_send.at[z], pass_recv.at[z], rows=mate)
    own.start()
    sent.append(own)
    for step in range(1, deep):
        to = ((z + step) % deep) * 2 + y
        copy = send(current_ref, gathered.at[row], own_send.at[step], own_recv.at[z], rows=to)
        copy.start()
        sent.append(copy)

    def multiply(value, source, first):
        for piece in range(n_cols):
            high = high_ref[source, piece * share:(piece + 1) * share, :]
            low = low_ref[source, piece * share:(piece + 1) * share, :]
            got = lax.dot_general(value, high, NT, preferred_element_type=jnp.float32)
            got = got + lax.dot_general(value, low, NT, preferred_element_type=jnp.float32)
            part[piece] = got if first else part[piece] + got

    for load in loads:
        load.wait()
    multiply(current_ref[...], row, True)
    for step in range(1, deep):
        other = (z + step) % deep
        source = other * 2 + y
        send(current_ref, gathered.at[source], own_send.at[step], own_recv.at[other], rows=mate).wait_recv()
        copy = send(gathered.at[source], gathered.at[source], pass_send.at[other], pass_recv.at[other], rows=mate)
        copy.start()
        sent.append(copy)
        multiply(gathered[source], source, False)
    for step in range(deep):
        other = (z + step) % deep
        source = other * 2 + 1 - y
        send(current_ref, gathered.at[source], pass_send.at[other], pass_recv.at[other], rows=mate).wait_recv()
        multiply(gathered[source], source, False)
    for copy in sent:
        copy.wait_send()

    twin = col + 1 - 2 * (col % 2)
    across = (col + 2) % 4
    twin_across = (twin + 2) % 4
    first = send(part.at[twin_across], came.at[1], part_send.at[1], part_recv.at[1], cols=twin)
    second = send(part.at[twin], came.at[0], part_send.at[0], part_recv.at[0], cols=twin)
    first.start()
    second.start()
    first.wait()
    came[3] = part[across] + came[1]
    third = send(came.at[3], came.at[2], part_send.at[2], part_recv.at[2], cols=across)
    third.start()
    second.wait()
    near = part[col] + came[0]
    third.wait()
    image = near + came[2]
    image_ref[...] = image

    gram = lax.dot_general(image, image, NT, precision=HIGHEST, preferred_element_type=jnp.float32)
    rest = width - LANES
    packed[0:width, :] = gram[:, 0:LANES]
    packed[width:width + rest, :] = jnp.zeros((rest, LANES), jnp.float32)
    packed[width:width + rest, 0:rest] = gram[LANES:width, LANES:width]
    piece_rows = (width + rest) // n_cols
    copies = []
    for step in range(1, n_cols):
        to = (col + step) % n_cols
        src = packed.at[pl.ds(pl.multiple_of(to * piece_rows, 8), piece_rows)]
        copy = send(src, gram_cols.at[col], gc_send.at[step], gc_recv.at[col], cols=to)
        copy.start()
        copies.append(copy)
    gram_cols[col] = packed[pl.ds(pl.multiple_of(col * piece_rows, 8), piece_rows), :]
    for step in range(1, n_cols):
        source = (col + step) % n_cols
        send(packed.at[pl.ds(0, piece_rows)], gram_cols.at[source], gc_send.at[step], gc_recv.at[source], cols=source).wait_recv()
    total = gram_cols[0]
    for piece in range(1, n_cols):
        total = total + gram_cols[piece]
    gram_rows[row] = total
    for step in range(1, n_rows):
        to = (row + step) % n_rows
        copy = send(gram_rows.at[row], gram_rows.at[row], gr_send.at[step], gr_recv.at[row], rows=to)
        copy.start()
        copies.append(copy)
    for step in range(1, n_rows):
        source = (row + step) % n_rows
        send(gram_rows.at[source], gram_rows.at[source], gr_send.at[step], gr_recv.at[source], rows=source).wait_recv()
    total = gram_rows[0]
    for piece in range(1, n_rows):
        total = total + gram_rows[piece]
    gram_whole[col] = total
    for step in range(1, n_cols):
        to = (col + step) % n_cols
        copy = send(gram_whole.at[col], gram_whole.at[col], gw_send.at[step], gw_recv.at[col], cols=to)
        copy.start()
        copies.append(copy)
    for step in range(1, n_cols):
        source = (col + step) % n_cols
        send(gram_whole.at[source], gram_whole.at[source], gw_send.at[step], gw_recv.at[source], cols=source).wait_recv()
    for piece in range(n_cols):
        gram_ref[piece * piece_rows:(piece + 1) * piece_rows, :] = gram_whole[piece]
    for copy in copies:
        copy.wait_send()


def image_step(n_rows, n_cols, current, high, low):
    width, share = current.shape
    lines = 2 * width - LANES
    piece = lines // n_cols
    vmem = pl.BlockSpec(memory_space=pltpu.VMEM)
    dma = pltpu.SemaphoreType.DMA
    f32 = jnp.float32
    return pl.pallas_call(
        functools.partial(image_kernel, n_rows, n_cols),
        out_shape=(jax.ShapeDtypeStruct((width, share), f32), jax.ShapeDtypeStruct((lines, LANES), f32)),
        in_specs=[vmem, pl.BlockSpec(memory_space=pl.ANY), pl.BlockSpec(memory_space=pl.ANY)],
        out_specs=(vmem, vmem),
        scratch_shapes=[
            pltpu.VMEM(high.shape, high.dtype),
            pltpu.VMEM(low.shape, low.dtype),
            dma((2,)),
            pltpu.VMEM((n_rows, width, share), jnp.bfloat16),
            pltpu.VMEM((n_cols, width, share), f32),
            pltpu.VMEM((4, width, share), f32),
            pltpu.VMEM((lines, LANES), f32),
            pltpu.VMEM((n_cols, piece, LANES), f32),
            pltpu.VMEM((n_rows, piece, LANES), f32),
            pltpu.VMEM((n_cols, piece, LANES), f32),
            dma((n_rows // 2,)), dma((n_rows // 2,)), dma((n_rows // 2,)), dma((n_rows // 2,)),
            dma((3,)), dma((3,)),
            dma((n_cols,)), dma((n_cols,)), dma((n_rows,)), dma((n_rows,)), dma((n_cols,)), dma((n_cols,)),
        ],
        compiler_params=pltpu.CompilerParams(
            collective_id=0, has_side_effects=True, vmem_limit_bytes=VMEM_BYTES
        ),
        name="image_step",
    )(current, high, low)


def solve_kernel(nodes, packed_ref, image_ref, solved_ref, rounded_ref, factor_ref, work):
    width = image_ref.shape[0]
    rest = width - LANES
    half = work.shape[1] // 2
    work[...] = jnp.zeros_like(work)
    work[:, 0:LANES] = packed_ref[0:width, :] / nodes
    work[0:LANES, LANES:width] = (packed_ref[LANES:width, :] / nodes).T
    work[LANES:width, LANES:width] = packed_ref[width:width + rest, 0:rest] / nodes
    row_ids = lax.broadcasted_iota(jnp.int32, (width, half), 0)
    col_ids = lax.broadcasted_iota(jnp.int32, (width, half), 1)
    work[:, half:] = (row_ids == col_ids).astype(jnp.float32)
    r_ids = lax.broadcasted_iota(jnp.int32, (BLOCK, LANES), 0)
    c_ids = lax.broadcasted_iota(jnp.int32, (BLOCK, LANES), 1)
    start = (r_ids == c_ids).astype(jnp.float32)
    lines = r_ids
    for first in range(0, width, BLOCK):
        last = first + BLOCK
        diag = work[first:last, first:last]
        columns = [jnp.broadcast_to(diag[:, k:k + 1], (BLOCK, LANES)) for k in range(BLOCK)]
        inverse = start
        for j in range(BLOCK):
            scale = jnp.where(lines > j, columns[j] * (1.0 / columns[j][j:j + 1, :]), 0.0)
            for k in range(j + 1, BLOCK):
                columns[k] = columns[k] - scale * columns[k][j:j + 1, :]
            inverse = inverse - scale * inverse[j:j + 1, :]
        pivots = columns[0]
        for k in range(1, BLOCK):
            pivots = jnp.where(lines == k, columns[k], pivots)
        inverse = (inverse / jnp.sqrt(pivots))[:, 0:BLOCK]
        panel = jnp.dot(inverse, work[first:last, :], precision=HIGHEST, preferred_element_type=jnp.float32)
        work[first:last, :] = panel
        if last < width:
            drop = lax.dot_general(panel[:, last:width], panel, TN, precision=HIGHEST, preferred_element_type=jnp.float32)
            work[last:width, :] = work[last:width, :] - drop
    factor = jnp.where(col_ids >= row_ids, work[:, 0:half], 0.0).T
    factor_ref[...] = factor[0:width, :]
    solved = jnp.dot(work[:, half:half + width], image_ref[...], precision=HIGHEST, preferred_element_type=jnp.float32)
    solved_ref[...] = solved
    rounded_ref[...] = solved.astype(jnp.bfloat16)


def solve_step(nodes, packed, image):
    width, share = image.shape
    vmem = pl.BlockSpec(memory_space=pltpu.VMEM)
    return pl.pallas_call(
        functools.partial(solve_kernel, nodes),
        out_shape=(
            jax.ShapeDtypeStruct((width, share), jnp.float32),
            jax.ShapeDtypeStruct((width, share), jnp.bfloat16),
            jax.ShapeDtypeStruct((width, width), jnp.float32),
        ),
        in_specs=[vmem, vmem],
        out_specs=(vmem, vmem, vmem),
        scratch_shapes=[pltpu.VMEM((width, 4 * LANES), jnp.float32)],
        compiler_params=pltpu.CompilerParams(vmem_limit_bytes=VMEM_BYTES),
        name="solve_step",
    )(packed, image)


def dense_shards(n_rows, n_cols, tile_values, tile_rows, tile_cols, tile_counts, sketch):
    tile = tile_values.shape[-1]
    pair = sketch.shape[0] // tile
    high, low = densify(tile_values[0, 0], tile_rows, tile_cols, tile_counts, n_rows, pair)
    current = sketch.T
    nodes = float(sketch.shape[0] * n_rows * n_cols)
    for power in range(POWER):
        image, packed = image_step(n_rows, n_cols, current, high, low)
        solved, current, factor = solve_step(nodes, packed, image)
    return (solved.T, factor)


def fits_dense(mesh, tile_values, sketch):
    n_rows, n_cols = mesh.shape["rows"], mesh.shape["cols"]
    tile = tile_values.shape[-1]
    share = sketch.shape[0] // (n_rows * n_cols)
    width = sketch.shape[1]
    dense = n_rows * share * RT * tile * 2
    lists = tile_values.shape[2] * tile * tile * 2
    return (
        n_cols == 4 and n_rows % 2 == 0 and tile == LANES and share % tile == 0
        and RT * tile == n_cols * share and LANES < width <= 2 * LANES and width % BLOCK == 0
        and (2 * width - LANES) % (8 * n_cols) == 0 and 2 * dense + lists < 40 * 1024 * 1024
    )


def accumulate(block_list, row_list, col_list, live_count, gathered, height):
    slot_total = block_list.shape[0]
    tile_size = block_list.shape[1]
    sketch_width = gathered.shape[1]
    tile_stack = gathered.reshape(-1, tile_size, sketch_width)
    block_size = math.gcd(32, slot_total)

    def one_block(block_index, running):
        first_slot = block_index * block_size
        block_values = lax.dynamic_slice_in_dim(block_list, first_slot, block_size, 0)
        rowids = lax.dynamic_slice_in_dim(row_list, first_slot, block_size, 0)
        colids = lax.dynamic_slice_in_dim(col_list, first_slot, block_size, 0)
        picked = jnp.take(tile_stack, colids, axis=0)
        products = jnp.einsum(
            "sab,sbk->sak", block_values, picked, preferred_element_type=jnp.float32
        )
        live_mask = (first_slot + jnp.arange(block_size, dtype=jnp.int32) < live_count).astype(
            jnp.float32
        )
        return running.at[rowids].add(products * live_mask[:, None, None])

    block_count = (live_count + block_size - 1) // block_size
    initial = jnp.zeros((height, tile_size, sketch_width), jnp.float32)
    running = lax.fori_loop(0, block_count, one_block, initial)
    return running.reshape(height * tile_size, sketch_width)


def shards(tile_values, tile_rows, tile_cols, tile_counts, sketch):
    own_values = tile_values[0, 0]
    own_rows = tile_rows[0, 0]
    own_cols = tile_cols[0, 0]
    own_count = tile_counts[0, 0]
    nodes_total = sketch.shape[0] * lax.axis_size("rows") * lax.axis_size("cols")
    current = sketch
    solved = None
    factor = None
    for power in range(POWER):
        gathered = lax.all_gather(current, "rows", axis=0, tiled=True)
        partial_value = accumulate(own_values, own_rows, own_cols, own_count, gathered, RT)
        whole = lax.psum(partial_value, "cols")
        gram_matrix = lax.psum(jnp.dot(whole.T, whole, precision=lax.Precision.HIGHEST), "rows")
        share_rows = whole.shape[0] // lax.axis_size("cols")
        owned = lax.dynamic_slice_in_dim(whole, lax.axis_index("cols") * share_rows, share_rows, 0)
        gram_matrix = gram_matrix / nodes_total
        factor = jnp.linalg.cholesky(gram_matrix)
        solved = lax.linalg.triangular_solve(
            factor, owned, left_side=False, lower=True, transpose_a=True
        )
        current = solved.astype(jnp.bfloat16)
    return (solved, factor)


def solution(mesh):
    placed = (
        P("rows", "cols", None, None, None),
        P("rows", "cols", None),
        P("rows", "cols", None),
        P("rows", "cols"),
        P(("rows", "cols"), None),
    )

    def run(*arrays):
        body = shards
        if fits_dense(mesh, arrays[0], arrays[4]):
            body = functools.partial(dense_shards, mesh.shape["rows"], mesh.shape["cols"])
        return jax.shard_map(
            body,
            mesh=mesh,
            in_specs=placed,
            out_specs=(P(("rows", "cols"), None), P()),
            check_vma=False,
        )(*arrays)

    return run
```
